32 devices in a mesh: row: 4 (over y, core), col: 8 (over z, x).
Axes of the slice: x: 2, y: 2, z: 4, core: 2. Of those that a mesh axis runs over, the one named last changes fastest.
Arguments:
- nodes: bfloat16 [256, 256, 128], P('row', 'col'), may hold values from -6 to 6
- edges: bfloat16 [4, 8, 16, 1024, 128], P('row', 'col'), may hold values from -2000 to 2000
- senders: int32 [4, 8, 16, 1024], P('row', 'col'), may hold values from 0 to 203, as said below
- receivers: int32 [4, 8, 16, 1024], P('row', 'col'), may hold values from 0 to 127, as said below
- counts: int32 [4, 8, 16], P('row', 'col'), may hold values from 512 to 1024, as said below
- w_edge_in: bfloat16 [384, 128], replicated, may hold values from -0.3125 to 0.3125
- w_edge_hid: bfloat16 [128, 128], replicated, may hold values from -0.5 to 0.5
- w_edge_out: bfloat16 [128, 128], replicated, may hold values from -0.5 to 0.5
- edge_bias: float32 [3, 128], replicated, may hold values from -3 to 3
- edge_gain: float32 [128], replicated, may hold values from 0.25 to 1.75
- edge_shift: float32 [128], replicated, may hold values from -3 to 3
- w_node_in: bfloat16 [256, 128], replicated, may hold values from -0.375 to 0.375
- w_node_hid: bfloat16 [128, 128], replicated, may hold values from -0.5 to 0.5
- w_node_out: bfloat16 [128, 128], replicated, may hold values from -0.5 to 0.5
- node_bias: float32 [3, 128], replicated, may hold values from -3 to 3
- node_gain: float32 [128], replicated, may hold values from 0.25 to 1.75
- node_shift: float32 [128], replicated, may hold values from -3 to 3
Outputs:
- new_nodes: bfloat16 [256, 256, 128], P('row', 'col')
- new_edges: bfloat16 [4, 8, 16, 1024, 128], P('row', 'col')
The draws below stay inside these ranges and needn't reach their ends.
Inputs may be any that keep to these rules, and one draw needn't show every extreme that they name: `senders`: the sender of slot k of band b is numbered in the window of node rows b * 4 - 1 to b * 4 + 4 and node columns -1 to 32 of its tile, row by row over 32 + 2 columns; it is one of the eight nodes around the receiver and lies inside the mesh. `receivers`: receivers are numbered row by row over the 4 x 32 nodes of the slot's band. Slots 0 to counts - 1 of a band hold edges, the others are empty; some band of every draw is full.
All inputs are finite; a program needn't handle non-finite values.
Results may differ from the reference program's by a relative error of at most 0.009.
Values may be sent and summed in bfloat16 or wider, within the bound.
A program may use at most 64 MiB of HBM per device.

```python
import jax
import jax.numpy as jnp
from jax import lax

L = 128
BR = 4
BANDS = 16
TC = 32
TR = 64
EDGE_SLOTS = 1024
TILES_R = 4
TILES_C = 8
NR = 256
NC = 256


def edge_geometry(key):
    local_key = jax.random.fold_in(key, 11)
    first_key, second_key = jax.random.split(local_key)
    shape = (TILES_R, TILES_C, BANDS, EDGE_SLOTS)
    recv_index = jax.random.randint(first_key, shape, 0, BR * TC, dtype=jnp.int32)
    direction = jax.random.randint(second_key, shape, 0, 8, dtype=jnp.int32)
    position = direction + (direction >= 4).astype(jnp.int32)
    step_row = position // 3 - 1
    step_col = position % 3 - 1
    tile_row = lax.broadcasted_iota(jnp.int32, shape, 0)
    tile_col = lax.broadcasted_iota(jnp.int32, shape, 1)
    band_index = lax.broadcasted_iota(jnp.int32, shape, 2)
    local_row = recv_index // TC
    local_col = recv_index % TC
    global_row = tile_row * (BANDS * BR) + band_index * BR + local_row
    global_col = tile_col * TC + local_col
    outside_row = (global_row + step_row < 0) | (global_row + step_row >= TILES_R * BANDS * BR)
    outside_col = (global_col + step_col < 0) | (global_col + step_col >= TILES_C * TC)
    step_row = jnp.where(outside_row, -step_row, step_row)
    step_col = jnp.where(outside_col, -step_col, step_col)
    send_index = (local_row + 1 + step_row) * (TC + 2) + local_col + 1 + step_col
    return (send_index.astype(jnp.int32), recv_index.astype(jnp.int32))


def draw_senders(key, part):
    return edge_geometry(key)[0]


def draw_receivers(key, part):
    return edge_geometry(key)[1]


def draw_counts(key, part):
    local_key = jax.random.fold_in(key, 23)
    first_key, second_key, third_key = jax.random.split(local_key, 3)
    shape = (TILES_R, TILES_C, BANDS)
    values = jax.random.randint(first_key, shape, EDGE_SLOTS // 2, EDGE_SLOTS + 1, dtype=jnp.int32)
    number = TILES_R * TILES_C * BANDS
    full_pick = jax.random.randint(second_key, (), 0, number, dtype=jnp.int32)
    least_pick = jax.random.randint(third_key, (), 0, number, dtype=jnp.int32)
    position = jnp.arange(number, dtype=jnp.int32).reshape(shape)
    values = jnp.where(position == least_pick, EDGE_SLOTS // 2, values)
    values = jnp.where(position == full_pick, EDGE_SLOTS, values)
    return values.astype(jnp.int32)


def draw_edges(key, part):
    local_key = jax.random.fold_in(key, 31)
    keys = jax.random.split(local_key, 5)
    shape = (TILES_R, TILES_C, BANDS, EDGE_SLOTS, L)
    row_part = jnp.arange(TILES_R, dtype=jnp.float32).reshape(TILES_R, 1, 1, 1, 1) / max(TILES_R - 1, 1)
    col_part = jnp.arange(TILES_C, dtype=jnp.float32).reshape(1, TILES_C, 1, 1, 1) / max(TILES_C - 1, 1)
    tile_scale = 1.0 + row_part + col_part
    row_scale = jnp.exp(jax.random.uniform(keys[0], (TILES_R, TILES_C, BANDS, EDGE_SLOTS, 1), jnp.float32, 0.0, jnp.log(10.0)))
    col_scale = jnp.exp(jax.random.uniform(keys[1], (L,), jnp.float32, 0.0, jnp.log(10.0)))
    noise = jnp.clip(jax.random.normal(keys[2], shape, jnp.float32), -4.0, 4.0)
    col_mean = 2.0 * jnp.clip(jax.random.normal(keys[4], (L,), jnp.float32), -3.0, 3.0) * col_scale
    row_offset = 6.0 * row_part * col_scale
    values = col_mean + row_offset + tile_scale * row_scale * col_scale * noise
    return values.astype(jnp.bfloat16)


def block_levels(own_key, extent, pieces, least, top_value):
    loudness, own = 1.0, jax.random.fold_in(own_key, 6)
    for dim, blocks in pieces:
        steps = jnp.exp(jax.random.uniform(jax.random.fold_in(own, dim), (blocks,), jnp.float32, least / len(pieces), top_value / len(pieces)))
        loudness = loudness * jnp.repeat(steps, extent[dim] // blocks).reshape([-1 if axis == dim else 1 for axis in range(len(extent))])
    return loudness


def normal_values(key, shape, scale, most, pieces=(), kind=jnp.bfloat16):
    values = jax.random.normal(key, shape, jnp.float32) * scale
    if len(pieces) > 0:
        values = block_levels(key, shape, pieces, -0.22, 0.18) * values
    return jnp.clip(values, min=-most, max=most).astype(kind)


def setup_inputs(seed: int = 0) -> dict:
    key_of = jax.random.split(jax.random.key(seed), 18)
    nodes = normal_values(key_of[0], (NR, NC, L), 1.0, 6.0, ((0, 4), (1, 8)))
    edges = draw_edges(jax.random.fold_in(key_of[17], 71), 0)
    senders = draw_senders(jax.random.fold_in(key_of[17], 71), 0)
    receivers = draw_receivers(jax.random.fold_in(key_of[17], 71), 0)
    counts = draw_counts(jax.random.fold_in(key_of[17], 71), 0)
    w_edge_in = normal_values(key_of[5], (3 * L, L), (3 * L) ** -0.5, 0.3125)
    w_edge_hid = normal_values(key_of[6], (L, L), L ** -0.5, 0.5)
    w_edge_out = normal_values(key_of[7], (L, L), L ** -0.5, 0.5)
    edge_bias = normal_values(key_of[8], (3, L), 0.5, 3.0, (), jnp.float32)
    edge_gain = jnp.clip(1.0 + 0.15 * jax.random.normal(key_of[9], (L,), jnp.float32), 0.25, 1.75)
    edge_shift = normal_values(key_of[10], (L,), 0.5, 3.0, (), jnp.float32)
    w_node_in = normal_values(key_of[11], (2 * L, L), (2 * L) ** -0.5, 0.375)
    w_node_hid = normal_values(key_of[12], (L, L), L ** -0.5, 0.5)
    w_node_out = normal_values(key_of[13], (L, L), L ** -0.5, 0.5)
    node_bias = normal_values(key_of[14], (3, L), 0.5, 3.0, (), jnp.float32)
    node_gain = jnp.clip(1.0 + 0.15 * jax.random.normal(key_of[15], (L,), jnp.float32), 0.25, 1.75)
    node_shift = normal_values(key_of[16], (L,), 0.5, 3.0, (), jnp.float32)
    return dict(nodes=nodes, edges=edges, senders=senders, receivers=receivers, counts=counts, w_edge_in=w_edge_in, w_edge_hid=w_edge_hid, w_edge_out=w_edge_out, edge_bias=edge_bias, edge_gain=edge_gain, edge_shift=edge_shift, w_node_in=w_node_in, w_node_hid=w_node_hid, w_node_out=w_node_out, node_bias=node_bias, node_gain=node_gain, node_shift=node_shift)


def layer_norm(values):
    centred = values - lax.optimization_barrier(jnp.mean(values, axis=-1, keepdims=True))
    spread = lax.optimization_barrier(jnp.mean(centred * centred, axis=-1, keepdims=True))
    return centred * lax.rsqrt(spread + 1e-05)

def reference(nodes, edges, senders, receivers, counts, w_edge_in, w_edge_hid, w_edge_out, edge_bias, edge_gain, edge_shift, w_node_in, w_node_hid, w_node_out, node_bias, node_gain, node_shift):
    tile_count = TILES_R * TILES_C
    latent = L
    flat_edges = edges.reshape(tile_count, BANDS, EDGE_SLOTS, latent)
    flat_send = senders.reshape(tile_count, BANDS, EDGE_SLOTS)
    flat_recv = receivers.reshape(tile_count, BANDS, EDGE_SLOTS)
    flat_count = counts.reshape(tile_count, BANDS)
    slot_index = jnp.arange(EDGE_SLOTS, dtype=jnp.int32)

    def live_of(count_row):
        return (slot_index[None, :] < count_row[:, None]).astype(jnp.float32)

    def first_pass(inputs):
        edge_block, count_row = inputs
        return lax.optimization_barrier(jnp.sum(edge_block.astype(jnp.float32) * live_of(count_row)[..., None], axis=(0, 1)))
    edge_total = jnp.sum(counts).astype(jnp.float32)
    edge_mean = lax.optimization_barrier(jnp.sum(lax.map(first_pass, (flat_edges, flat_count)), axis=0)) / edge_total

    def second_pass(inputs):
        edge_block, count_row = inputs
        centred = edge_block.astype(jnp.float32) - edge_mean
        return lax.optimization_barrier(jnp.sum(centred * centred * live_of(count_row)[..., None], axis=(0, 1)))
    edge_var = lax.optimization_barrier(jnp.sum(lax.map(second_pass, (flat_edges, flat_count)), axis=0)) / edge_total
    inv_spread = lax.rsqrt(edge_var + 1e-05)
    padded = jnp.pad(nodes, ((1, 1), (1, 1), (0, 0)))
    send_base = (jnp.arange(BANDS, dtype=jnp.int32) * (BR * (TC + 2)))[:, None]
    recv_base = (jnp.arange(BANDS, dtype=jnp.int32) * (BR * TC))[:, None]
    zero_index = jnp.zeros((), jnp.int32)

    def tile_step(inputs):
        tile_id, edge_block, send_index, recv_index, count_row = inputs
        tile_row = (tile_id // TILES_C).astype(jnp.int32)
        tile_col = (tile_id % TILES_C).astype(jnp.int32)
        window = lax.dynamic_slice(padded, (tile_row * TR, tile_col * TC, zero_index), (TR + 2, TC + 2, latent)).reshape(-1, latent)
        own_nodes = lax.dynamic_slice(nodes, (tile_row * TR, tile_col * TC, zero_index), (TR, TC, latent)).reshape(-1, latent)
        sender_lat = window[(send_index + send_base).reshape(-1)]
        receiver_index = (recv_index + recv_base).reshape(-1).astype(jnp.int32)
        receiver_lat = own_nodes[receiver_index]
        normed = ((edge_block.reshape(-1, latent).astype(jnp.float32) - edge_mean) * inv_spread).astype(jnp.bfloat16)
        joined = jnp.concatenate([normed, sender_lat, receiver_lat], axis=1)
        hidden_one = jax.nn.relu(jnp.dot(joined, w_edge_in, preferred_element_type=jnp.float32) + edge_bias[0]).astype(jnp.bfloat16)
        hidden_two = jax.nn.relu(jnp.dot(hidden_one, w_edge_hid, preferred_element_type=jnp.float32) + edge_bias[1]).astype(jnp.bfloat16)
        message = jnp.dot(hidden_two, w_edge_out, preferred_element_type=jnp.float32) + edge_bias[2]
        live_mask = live_of(count_row).reshape(-1, 1)
        fresh = (live_mask * (normed.astype(jnp.float32) + layer_norm(message) * edge_gain + edge_shift)).astype(jnp.bfloat16)
        gathered = jax.ops.segment_sum(fresh.astype(jnp.float32), receiver_index, num_segments=TR * TC).astype(jnp.bfloat16)
        node_input = jnp.concatenate([own_nodes, gathered], axis=1)
        node_one = jax.nn.relu(jnp.dot(node_input, w_node_in, preferred_element_type=jnp.float32) + node_bias[0]).astype(jnp.bfloat16)
        node_two = jax.nn.relu(jnp.dot(node_one, w_node_hid, preferred_element_type=jnp.float32) + node_bias[1]).astype(jnp.bfloat16)
        node_message = jnp.dot(node_two, w_node_out, preferred_element_type=jnp.float32) + node_bias[2]
        updated = (own_nodes.astype(jnp.float32) + layer_norm(node_message) * node_gain + node_shift).astype(jnp.bfloat16)
        return (fresh.reshape(BANDS, EDGE_SLOTS, latent), updated.reshape(TR, TC, latent))
    tile_ids = jnp.arange(tile_count, dtype=jnp.int32)
    fresh_edges, fresh_tiles = lax.map(tile_step, (tile_ids, flat_edges, flat_send, flat_recv, flat_count))
    new_edges = fresh_edges.reshape(TILES_R, TILES_C, BANDS, EDGE_SLOTS, latent)
    new_nodes = fresh_tiles.reshape(TILES_R, TILES_C, TR, TC, latent).transpose(0, 2, 1, 3, 4).reshape(NR, NC, latent)
    return (new_nodes, new_edges)
```

```python
import functools

import jax
import jax.numpy as jnp
from jax import lax
from jax.experimental import pallas as pl
from jax.experimental.pallas import tpu as pltpu
from jax.sharding import PartitionSpec as P

MESH = pl.DeviceIdType.MESH
EPS = 1e-05
TAIL = 16
F32 = jnp.float32
BF16 = jnp.bfloat16
VMEM = pl.BlockSpec(memory_space=pltpu.VMEM)
SMEM = pl.BlockSpec(memory_space=pltpu.SMEM)
ANY = pl.BlockSpec(memory_space=pl.ANY)


def dot(a, b):
    return jnp.dot(a, b, preferred_element_type=F32)


def stats_kernel(bands_step, counts, edges, stats, acc_sum, acc_sq, shift):
    step = pl.program_id(0)
    slots, latent = edges.shape[1:]

    @pl.when(step == 0)
    def _():
        shift[...] = jnp.broadcast_to(edges[0, 0:TAIL, :].astype(F32)[0:1], shift.shape)
        acc_sum[...] = jnp.zeros_like(acc_sum)
        acc_sq[...] = jnp.zeros_like(acc_sq)

    base = shift[0:1, :]
    total, square = acc_sum[...], acc_sq[...]
    for k in range(bands_step):
        count = counts[step * bands_step + k]
        rows = lax.broadcasted_iota(jnp.int32, (slots, latent), 0)
        moved = jnp.where(rows < count, edges[k].astype(F32) - base, 0.0)
        total += jnp.sum(moved.reshape(-1, 8, latent), axis=0)
        square += jnp.sum((moved * moved).reshape(-1, 8, latent), axis=0)
    acc_sum[...] = total
    acc_sq[...] = square

    @pl.when(step == pl.num_programs(0) - 1)
    def _():
        number = counts[0]
        for k in range(1, counts.shape[0]):
            number = number + counts[k]
        number = jnp.full((1, latent), number.astype(F32))
        first = jnp.sum(acc_sum[...], axis=0, keepdims=True)
        second = jnp.sum(acc_sq[...], axis=0, keepdims=True)
        offset = first / number
        stats[0:1, :] = base + offset
        stats[1:2, :] = second - first * offset
        stats[2:3, :] = number
        stats[3:8, :] = jnp.zeros((5, latent), F32)


def combine(tiles):
    number = sum(tile[2:3] for tile in tiles)
    mean = sum(tile[2:3] * tile[0:1] for tile in tiles) / number
    power = sum(tile[1:2] + tile[2:3] * (tile[0:1] - mean) * (tile[0:1] - mean) for tile in tiles)
    return mean, power, number


def exchange_kernel(
    num_rows, num_cols, stats, row_edge, col_edge, norm, halo_row, halo_col,
    first, middle, second, send_sem, recv_sem, stat_send, stat_recv,
):
    r, c = lax.axis_index("row"), lax.axis_index("col")

    def at(dr, dc):
        return (lax.rem(r + dr + num_rows, num_rows), lax.rem(c + dc + num_cols, num_cols))

    near = [(0, k) for k in range(1, num_cols)] + [(k, 0) for k in range(1, num_rows)]
    peers = near + [(1, 1), (1, -1), (-1, 1), (-1, -1)]
    barrier = pltpu.get_barrier_semaphore()
    for dr, dc in peers:
        pl.semaphore_signal(barrier, inc=1, device_id=at(dr, dc), device_id_type=MESH)
    pl.semaphore_wait(barrier, len(peers))

    def send(src, dst, ss, rs, dr, dc):
        copy = pltpu.make_async_remote_copy(
            src_ref=src, dst_ref=dst, send_sem=ss, recv_sem=rs,
            device_id=at(dr, dc), device_id_type=MESH,
        )
        copy.start()
        return copy

    stage = [
        send(stats, first.at[k - 1], stat_send.at[k - 1], stat_recv.at[k - 1], 0, k)
        for k in range(1, num_cols)
    ]
    length = col_edge.shape[1]
    top, low = pl.ds(0, TAIL), pl.ds(length - TAIL, TAIL)
    plan = [
        (col_edge.at[1], halo_col.at[0, pl.ds(TAIL, length)], 0, 1),
        (col_edge.at[0], halo_col.at[1, pl.ds(TAIL, length)], 0, -1),
        (row_edge.at[1], halo_row.at[0], 1, 0),
        (row_edge.at[0], halo_row.at[1], -1, 0),
        (col_edge.at[1, low], halo_col.at[0, top], 1, 1),
        (col_edge.at[1, top], halo_col.at[0, pl.ds(TAIL + length, TAIL)], -1, 1),
        (col_edge.at[0, low], halo_col.at[1, top], 1, -1),
        (col_edge.at[0, top], halo_col.at[1, pl.ds(TAIL + length, TAIL)], -1, -1),
    ]
    halo = [
        send(src, dst, send_sem.at[i], recv_sem.at[i], dr, dc)
        for i, (src, dst, dr, dc) in enumerate(plan)
    ]
    for copy in stage:
        copy.wait()
    mean, power, number = combine([stats[...]] + [first[k] for k in range(num_cols - 1)])
    latent = stats.shape[1]
    middle[...] = jnp.concatenate([mean, power, number, jnp.zeros((5, latent), F32)], axis=0)
    base = num_cols - 1
    stage = [
        send(middle, second.at[k - 1], stat_send.at[base + k - 1], stat_recv.at[base + k - 1], k, 0)
        for k in range(1, num_rows)
    ]
    for copy in stage:
        copy.wait()
    mean, power, number = combine([middle[...]] + [second[k] for k in range(num_rows - 1)])
    spread = lax.rsqrt(power / number + EPS)
    norm[...] = jnp.concatenate([mean, spread, jnp.zeros((6, latent), F32)], axis=0)
    for copy in halo:
        copy.wait()


def twice(w):
    zero = jnp.zeros_like(w)
    return jnp.concatenate(
        [jnp.concatenate([w, zero], axis=1), jnp.concatenate([zero, w], axis=1)], axis=0
    )


def centred(w):
    wide = w.astype(F32)
    return wide - jnp.mean(wide, axis=-1, keepdims=True)


def main_kernel(
    band_rows, cols, counts, edges, send_all, recv_all, nodes, halo_row, halo_col, norm,
    w_in, w_hid, w_out, bias, gain, shift, v_in, v_hid, v_out, n_bias, n_gain, n_shift,
    new_edges, new_nodes,
    proj_send, proj_left, proj_right, proj_recv, mixed, two_hid, two_out, two_mean, gathered,
):
    band = pl.program_id(0)
    slots, latent = edges.shape[1:]
    band_nodes = band_rows * cols
    window_rows = band_rows + 2
    main = window_rows * cols
    table = mixed.shape[0] - band_nodes - latent
    half = slots // 2

    @pl.when(band == 0)
    def _():
        w_send = w_in[latent : 2 * latent, :]
        w_recv = w_in[2 * latent :, :]
        total = nodes.shape[0]
        proj_send[0:cols, :] = dot(halo_row[0], w_send).astype(BF16)
        proj_send[cols : cols + total, :] = dot(nodes[...], w_send).astype(BF16)
        proj_send[cols + total :, :] = dot(halo_row[1], w_send).astype(BF16)
        proj_left[...] = dot(halo_col[0], w_send)
        proj_right[...] = dot(halo_col[1], w_send)
        proj_recv[...] = (dot(nodes[...], w_recv) + bias[0:1, :]).astype(BF16)
        mixed[...] = jnp.zeros_like(mixed)
        mixed[table + band_nodes :, :] = w_in[0:latent, :]
        two_hid[...] = twice(w_hid[...])
        two_out[...] = twice(centred(w_out[...]).astype(BF16))
        two_mean[...] = twice(jnp.full((latent, latent), 1.0 / latent, BF16))

    start = pl.multiple_of(band * band_nodes, band_nodes)
    side = TAIL - 1 + band * band_rows
    mixed[0:main, :] = proj_send[pl.ds(start, main), :]
    mixed[main : main + 16, :] = jnp.concatenate(
        [proj_left[pl.ds(side, 8), :], proj_right[pl.ds(side, 8), :]], axis=0
    ).astype(BF16)
    mixed[table : table + band_nodes, :] = proj_recv[pl.ds(start, band_nodes), :]
    weights = mixed[...]

    send = send_all[pl.ds(band, 1), :]
    recv = recv_all[pl.ds(band, 1), :]
    row = sum((send >= (cols + 2) * k).astype(jnp.int32) for k in range(1, window_rows))
    col = send - (cols + 2) * row
    place = jnp.where(
        col == 0, main + row, jnp.where(col == cols + 1, main + 8 + row, row * cols + col - 1)
    )
    count = counts[band]
    mean, spread = norm[0:1, :], norm[1:2, :]
    bias_hid = jnp.concatenate([bias[1:2, :]] * 2, axis=1)
    bias_msg = bias[2:3, :] - jnp.mean(bias[2:3, :], axis=-1, keepdims=True)
    bias_out = jnp.concatenate([bias_msg] * 2, axis=1)

    def spread_rows(index, lo):
        return jnp.broadcast_to(index[:, lo : lo + 128], (128, 128)).T

    def pick(values, width, offset=0):
        lanes = lax.broadcasted_iota(jnp.int32, (values.shape[0], width), 1) + offset
        return jnp.where(values == lanes, 1.0, 0.0).astype(BF16)

    ones, normed = [], []
    for part in range(2):
        pieces = []
        for lo in range(part * half, (part + 1) * half, 128):
            s, q = spread_rows(place, lo), spread_rows(recv, lo)
            hot = [pick(s, 128, off) for off in range(0, table, 128)]
            hot += [pick(q, 128, off) for off in range(0, band_nodes, 128)]
            pieces.append(jnp.concatenate(hot, axis=1))
        hot = jnp.concatenate(pieces, axis=0)
        block = edges[0, part * half : (part + 1) * half, :].astype(F32)
        value = ((block - mean) * spread).astype(BF16)
        normed.append(value)
        joined = jnp.concatenate([hot, value], axis=1)
        ones.append(jnp.maximum(dot(joined, weights), 0.0).astype(BF16))
    one = jnp.concatenate(ones, axis=1)
    two = jnp.maximum(dot(one, two_hid[...]) + bias_hid, 0.0).astype(BF16)
    message = dot(two, two_out[...]) + bias_out
    power = dot((message * message).astype(BF16), two_mean[...])
    unit = message * lax.rsqrt(power + EPS)
    fresh = []
    for part in range(2):
        rows = lax.broadcasted_iota(jnp.int32, (half, latent), 0) + part * half
        value = normed[part].astype(F32) + unit[:, part * latent : (part + 1) * latent] * gain[...] + shift[...]
        value = jnp.where(rows < count, value, 0.0).astype(BF16)
        new_edges[0, part * half : (part + 1) * half, :] = value
        fresh.append(value)
    fresh = jnp.concatenate(fresh, axis=0)
    places = lax.broadcasted_iota(jnp.int32, (band_nodes, slots), 0)
    pick_recv = jnp.where(places == recv, 1.0, 0.0).astype(BF16)
    gathered[pl.ds(start, band_nodes), :] = dot(pick_recv, fresh).astype(BF16)

    @pl.when(band == pl.num_programs(0) - 1)
    def _():
        own = nodes[...]
        joined = jnp.concatenate([own, gathered[...]], axis=1)
        node_one = jnp.maximum(dot(joined, v_in[...]) + n_bias[0:1, :], 0.0).astype(BF16)
        node_two = jnp.maximum(dot(node_one, v_hid[...]) + n_bias[1:2, :], 0.0).astype(BF16)
        out_bias = n_bias[2:3, :] - jnp.mean(n_bias[2:3, :], axis=-1, keepdims=True)
        note = dot(node_two, centred(v_out[...]).astype(BF16)) + out_bias
        level = dot((note * note).astype(BF16), jnp.full((latent, latent), 1.0 / latent, BF16))
        value = own.astype(F32) + note * lax.rsqrt(level + EPS) * n_gain[...] + n_shift[...]
        new_nodes[...] = value.astype(BF16)


def round_up(value, unit):
    return -(-value // unit) * unit


def per_device(
    nodes, edges, senders, receivers, counts, w_edge_in, w_edge_hid, w_edge_out, edge_bias,
    edge_gain, edge_shift, w_node_in, w_node_hid, w_node_out, node_bias, node_gain, node_shift,
):
    rows, cols, latent = nodes.shape
    bands, slots = edges.shape[2:4]
    band_rows = rows // bands
    num_rows, num_cols = lax.axis_size("row"), lax.axis_size("col")
    tile_edges = edges.reshape(bands, slots, latent)
    tile_send = senders.reshape(bands, slots)
    tile_recv = receivers.reshape(bands, slots)
    tile_counts = counts.reshape(bands)
    flat = nodes.reshape(rows * cols, latent)

    step = 2 if bands % 2 == 0 else 1
    stats = pl.pallas_call(
        functools.partial(stats_kernel, step),
        grid=(bands // step,),
        in_specs=[SMEM, pl.BlockSpec((step, slots, latent), lambda i: (i, 0, 0))],
        out_specs=VMEM,
        out_shape=jax.ShapeDtypeStruct((8, latent), F32),
        scratch_shapes=[pltpu.VMEM((8, latent), F32)] * 3,
        name="stats",
    )(tile_counts, tile_edges)

    row_edge = jnp.stack([nodes[0], nodes[-1]])
    col_edge = jnp.stack([nodes[:, 0], nodes[:, -1]])
    stages = num_cols + num_rows - 2
    norm, halo_row, halo_col = pl.pallas_call(
        functools.partial(exchange_kernel, num_rows, num_cols),
        in_specs=[VMEM] * 3,
        out_specs=[VMEM] * 3,
        out_shape=[
            jax.ShapeDtypeStruct((8, latent), F32),
            jax.ShapeDtypeStruct((2, cols, latent), BF16),
            jax.ShapeDtypeStruct((2, rows + 2 * TAIL, latent), BF16),
        ],
        scratch_shapes=[
            pltpu.VMEM((max(num_cols - 1, 1), 8, latent), F32),
            pltpu.VMEM((8, latent), F32),
            pltpu.VMEM((max(num_rows - 1, 1), 8, latent), F32),
            pltpu.SemaphoreType.DMA((8,)),
            pltpu.SemaphoreType.DMA((8,)),
            pltpu.SemaphoreType.DMA((stages,)),
            pltpu.SemaphoreType.DMA((stages,)),
        ],
        compiler_params=pltpu.CompilerParams(collective_id=0, has_side_effects=True),
        name="exchange",
    )(stats, row_edge, col_edge)

    band_nodes = band_rows * cols
    table = round_up((band_rows + 2) * cols + 16, 128)
    out_edges, out_nodes = pl.pallas_call(
        functools.partial(main_kernel, band_rows, cols),
        grid=(bands,),
        in_specs=[SMEM, pl.BlockSpec((1, slots, latent), lambda i: (i, 0, 0))] + [VMEM] * 18,
        out_specs=[pl.BlockSpec((1, slots, latent), lambda i: (i, 0, 0)), VMEM],
        out_shape=[
            jax.ShapeDtypeStruct((bands, slots, latent), BF16),
            jax.ShapeDtypeStruct((rows * cols, latent), BF16),
        ],
        scratch_shapes=[
            pltpu.VMEM(((rows + 2) * cols, latent), BF16),
            pltpu.VMEM((rows + 2 * TAIL, latent), F32),
            pltpu.VMEM((rows + 2 * TAIL, latent), F32),
            pltpu.VMEM((rows * cols, latent), BF16),
            pltpu.VMEM((table + band_nodes + latent, latent), BF16),
            pltpu.VMEM((2 * latent, 2 * latent), BF16),
            pltpu.VMEM((2 * latent, 2 * latent), BF16),
            pltpu.VMEM((2 * latent, 2 * latent), BF16),
            pltpu.VMEM((rows * cols, latent), BF16),
        ],
        name="processor",
    )(
        tile_counts, tile_edges, tile_send, tile_recv, flat, halo_row, halo_col, norm,
        w_edge_in, w_edge_hid, w_edge_out, edge_bias, edge_gain.reshape(1, latent),
        edge_shift.reshape(1, latent), w_node_in, w_node_hid, w_node_out, node_bias,
        node_gain.reshape(1, latent), node_shift.reshape(1, latent),
    )
    return out_nodes.reshape(rows, cols, latent), out_edges.reshape(edges.shape)


def solution(mesh):
    tile = ("row", "col")
    in_specs = (
        P(*tile, None),
        P(*tile, None, None, None),
        P(*tile, None, None),
        P(*tile, None, None),
        P(*tile, None),
    ) + (P(),) * 12
    out_specs = (P(*tile, None), P(*tile, None, None, None))
    return jax.shard_map(
        per_device, mesh=mesh, in_specs=in_specs, out_specs=out_specs, check_vma=False
    )
```

```python
import functools

import jax
import jax.numpy as jnp
from jax import lax
from jax.experimental import pallas as pl
from jax.experimental.pallas import tpu as pltpu
from jax.sharding import PartitionSpec as P

MESH = pl.DeviceIdType.MESH
EPS = 1e-05
TAIL = 16
F32 = jnp.float32
BF16 = jnp.bfloat16
VMEM = pl.BlockSpec(memory_space=pltpu.VMEM)
SMEM = pl.BlockSpec(memory_space=pltpu.SMEM)
ANY = pl.BlockSpec(memory_space=pl.ANY)


def dot(a, b):
    return jnp.dot(a, b, preferred_element_type=F32)


def combine(tiles, latent):
    parts = [[tile[:, k * latent : (k + 1) * latent] for k in range(3)] for tile in tiles]
    number = sum(n for _, _, n in parts)
    mean = sum(n * m for m, _, n in parts) / number
    power = sum(p + n * (m - mean) * (m - mean) for m, p, n in parts)
    return mean, power, number


def exchange_kernel(
    num_rows, num_cols, bands_step, counts, edges, nodes, norm, row_out, col_out,
    halo_row, halo_col, acc_sum, acc_sq, shift, col_edge, stats, first, middle, second,
    send_sem, recv_sem, stat_send, stat_recv,
):
    step, steps = pl.program_id(0), pl.num_programs(0)
    r, c = lax.axis_index("row"), lax.axis_index("col")
    slots, latent = edges.shape[1:]
    length, cols = nodes.shape[0:2]

    def at(dr, dc):
        return (lax.rem(r + dr + num_rows, num_rows), lax.rem(c + dc + num_cols, num_cols))

    near = [(0, k) for k in range(1, num_cols)] + [(k, 0) for k in range(1, num_rows)]
    peers = near + [(1, 1), (1, -1), (-1, 1), (-1, -1)]
    barrier = pltpu.get_barrier_semaphore()

    def copy_of(src, dst, ss, rs, dr, dc):
        return pltpu.make_async_remote_copy(
            src_ref=src, dst_ref=dst, send_sem=ss, recv_sem=rs,
            device_id=at(dr, dc), device_id_type=MESH,
        )

    top, low = pl.ds(0, TAIL), pl.ds(length - TAIL, TAIL)
    plan = [
        (col_edge.at[1], halo_col.at[0, pl.ds(TAIL, length)], 0, 1),
        (col_edge.at[0], halo_col.at[1, pl.ds(TAIL, length)], 0, -1),
        (nodes.at[length - 1], halo_row.at[0], 1, 0),
        (nodes.at[0], halo_row.at[1], -1, 0),
        (col_edge.at[1, low], halo_col.at[0, top], 1, 1),
        (col_edge.at[1, top], halo_col.at[0, pl.ds(TAIL + length, TAIL)], -1, 1),
        (col_edge.at[0, low], halo_col.at[1, top], 1, -1),
        (col_edge.at[0, top], halo_col.at[1, pl.ds(TAIL + length, TAIL)], -1, -1),
    ]

    def halo():
        return [
            copy_of(src, dst, send_sem.at[i], recv_sem.at[i], dr, dc)
            for i, (src, dst, dr, dc) in enumerate(plan)
        ]

    @pl.when(step == 0)
    def _():
        for dr, dc in peers:
            pl.semaphore_signal(barrier, inc=1, device_id=at(dr, dc), device_id_type=MESH)
        shift[...] = jnp.broadcast_to(edges[0, 0:TAIL, :].astype(F32)[0:1], shift.shape)
        acc_sum[...] = jnp.zeros_like(acc_sum)
        acc_sq[...] = jnp.zeros_like(acc_sq)
        flat = nodes[...].reshape(length * cols, latent)
        line = lax.broadcasted_iota(jnp.int32, (length, length * cols), 0) * cols
        place = lax.broadcasted_iota(jnp.int32, (length, length * cols), 1)
        for side, offset in enumerate((0, cols - 1)):
            pick = jnp.where(place == line + offset, 1.0, 0.0).astype(BF16)
            col_edge[side] = dot(pick, flat).astype(BF16)

    @pl.when(step == steps // 2)
    def _():
        pl.semaphore_wait(barrier, len(peers))
        for copy in halo():
            copy.start()

    base = shift[0:1, :]
    total, square = acc_sum[...], acc_sq[...]
    group = 64
    for k in range(bands_step):
        count = counts[step * bands_step + k]
        for lo in range(0, slots, group):
            moved = edges[k, lo : lo + group, :].astype(F32) - base
            if lo + group > slots // 2:
                rows = lax.broadcasted_iota(jnp.int32, (group, latent), 0) + lo
                moved = jnp.where(rows < count, moved, 0.0)
            total += jnp.sum(moved.reshape(-1, 8, latent), axis=0)
            square += jnp.sum((moved * moved).reshape(-1, 8, latent), axis=0)
    acc_sum[...] = total
    acc_sq[...] = square

    @pl.when(step == steps - 1)
    def _():
        amount = counts[0]
        for k in range(1, counts.shape[0]):
            amount = amount + counts[k]
        amount = jnp.full((1, latent), amount.astype(F32))
        offset = jnp.sum(acc_sum[...], axis=0, keepdims=True) / amount
        spare = jnp.sum(acc_sq[...], axis=0, keepdims=True) - offset * offset * amount
        stats[...] = jnp.concatenate([base + offset, spare, amount], axis=1)
        stage = [
            copy_of(stats, first.at[k - 1], stat_send.at[k - 1], stat_recv.at[k - 1], 0, k)
            for k in range(1, num_cols)
        ]
        for copy in stage:
            copy.start()
        for copy in stage:
            copy.wait()
        merged = combine([stats[...]] + [first[k] for k in range(num_cols - 1)], latent)
        middle[...] = jnp.concatenate(merged, axis=1)
        past = num_cols - 1
        stage = [
            copy_of(
                middle, second.at[k - 1], stat_send.at[past + k - 1],
                stat_recv.at[past + k - 1], k, 0,
            )
            for k in range(1, num_rows)
        ]
        for copy in stage:
            copy.start()
        for copy in halo():
            copy.wait()
        row_out[...] = halo_row[...]
        col_out[...] = halo_col[...]
        for copy in stage:
            copy.wait()
        mean, power, number = combine(
            [middle[...]] + [second[k] for k in range(num_rows - 1)], latent
        )
        spread = lax.rsqrt(jnp.maximum(power / number, 0.0) + EPS)
        norm[...] = jnp.concatenate([mean, spread, jnp.zeros((6, latent), F32)], axis=0)


def twice(w):
    zero = jnp.zeros_like(w)
    return jnp.concatenate(
        [jnp.concatenate([w, zero], axis=1), jnp.concatenate([zero, w], axis=1)], axis=0
    )


def centred(w):
    wide = w.astype(F32)
    return wide - jnp.mean(wide, axis=-1, keepdims=True)


def main_kernel(
    band_rows, cols, counts, edges, send_all, recv_all, nodes, halo_row, halo_col, norm,
    w_in, w_hid, w_out, bias, gain, shift, v_in, v_hid, v_out, n_bias, n_gain, n_shift,
    new_edges, new_nodes,
    proj_send, proj_left, proj_right, proj_recv, mixed, two_hid, two_out, two_mean, gathered,
):
    band = pl.program_id(0)
    slots, latent = edges.shape[1:]
    band_nodes = band_rows * cols
    window_rows = band_rows + 2
    main = window_rows * cols
    table = mixed.shape[0] - band_nodes - latent
    half = slots // 2

    @pl.when(band == 0)
    def _():
        w_send = w_in[latent : 2 * latent, :]
        w_recv = w_in[2 * latent :, :]
        total = nodes.shape[0]
        proj_send[0:cols, :] = dot(halo_row[0], w_send).astype(BF16)
        proj_send[cols : cols + total, :] = dot(nodes[...], w_send).astype(BF16)
        proj_send[cols + total :, :] = dot(halo_row[1], w_send).astype(BF16)
        proj_left[...] = dot(halo_col[0], w_send)
        proj_right[...] = dot(halo_col[1], w_send)
        proj_recv[...] = (dot(nodes[...], w_recv) + bias[0:1, :]).astype(BF16)
        mixed[...] = jnp.zeros_like(mixed)
        mixed[table + band_nodes :, :] = w_in[0:latent, :]
        two_hid[...] = twice(w_hid[...])
        two_out[...] = twice(centred(w_out[...]).astype(BF16))
        two_mean[...] = twice(jnp.full((latent, latent), 1.0 / latent, BF16))

    start = pl.multiple_of(band * band_nodes, band_nodes)
    side = TAIL - 1 + band * band_rows
    mixed[0:main, :] = proj_send[pl.ds(start, main), :]
    mixed[main : main + 16, :] = jnp.concatenate(
        [proj_left[pl.ds(side, 8), :], proj_right[pl.ds(side, 8), :]], axis=0
    ).astype(BF16)
    mixed[table : table + band_nodes, :] = proj_recv[pl.ds(start, band_nodes), :]
    weights = mixed[...]

    send = send_all[pl.ds(band, 1), :]
    recv = recv_all[pl.ds(band, 1), :]
    row = sum((send >= (cols + 2) * k).astype(jnp.int32) for k in range(1, window_rows))
    col = send - (cols + 2) * row
    place = jnp.where(
        col == 0, main + row, jnp.where(col == cols + 1, main + 8 + row, row * cols + col - 1)
    )
    count = counts[band]
    mean, spread = norm[0:1, :], norm[1:2, :]
    bias_hid = jnp.concatenate([bias[1:2, :]] * 2, axis=1)
    bias_msg = bias[2:3, :] - jnp.mean(bias[2:3, :], axis=-1, keepdims=True)
    bias_out = jnp.concatenate([bias_msg] * 2, axis=1)

    def spread_rows(index, lo):
        return jnp.broadcast_to(index[:, lo : lo + 128], (128, 128)).T

    def pick(values, width, offset=0):
        lanes = lax.broadcasted_iota(jnp.int32, (values.shape[0], width), 1) + offset
        return jnp.where(values == lanes, 1.0, 0.0).astype(BF16)

    ones, normed = [], []
    for part in range(2):
        pieces = []
        for lo in range(part * half, (part + 1) * half, 128):
            s, q = spread_rows(place, lo), spread_rows(recv, lo)
            hot = [pick(s, 128, off) for off in range(0, table, 128)]
            hot += [pick(q, 128, off) for off in range(0, band_nodes, 128)]
            pieces.append(jnp.concatenate(hot, axis=1))
        hot = jnp.concatenate(pieces, axis=0)
        block = edges[0, part * half : (part + 1) * half, :].astype(F32)
        value = ((block - mean) * spread).astype(BF16)
        normed.append(value)
        joined = jnp.concatenate([hot, value], axis=1)
        ones.append(jnp.maximum(dot(joined, weights), 0.0).astype(BF16))
    one = jnp.concatenate(ones, axis=1)
    two = jnp.maximum(dot(one, two_hid[...]) + bias_hid, 0.0).astype(BF16)
    message = dot(two, two_out[...]) + bias_out
    power = dot((message * message).astype(BF16), two_mean[...])
    unit = message * lax.rsqrt(power + EPS)
    fresh = []
    for part in range(2):
        rows = lax.broadcasted_iota(jnp.int32, (half, latent), 0) + part * half
        value = normed[part].astype(F32) + unit[:, part * latent : (part + 1) * latent] * gain[...] + shift[...]
        value = jnp.where(rows < count, value, 0.0).astype(BF16)
        new_edges[0, part * half : (part + 1) * half, :] = value
        fresh.append(value)
    fresh = jnp.concatenate(fresh, axis=0)
    places = lax.broadcasted_iota(jnp.int32, (band_nodes, slots), 0)
    pick_recv = jnp.where(places == recv, 1.0, 0.0).astype(BF16)
    gathered[pl.ds(start, band_nodes), :] = dot(pick_recv, fresh).astype(BF16)

    @pl.when(band == pl.num_programs(0) - 1)
    def _():
        own = nodes[...]
        joined = jnp.concatenate([own, gathered[...]], axis=1)
        node_one = jnp.maximum(dot(joined, v_in[...]) + n_bias[0:1, :], 0.0).astype(BF16)
        node_two = jnp.maximum(dot(node_one, v_hid[...]) + n_bias[1:2, :], 0.0).astype(BF16)
        out_bias = n_bias[2:3, :] - jnp.mean(n_bias[2:3, :], axis=-1, keepdims=True)
        note = dot(node_two, centred(v_out[...]).astype(BF16)) + out_bias
        level = dot((note * note).astype(BF16), jnp.full((latent, latent), 1.0 / latent, BF16))
        value = own.astype(F32) + note * lax.rsqrt(level + EPS) * n_gain[...] + n_shift[...]
        new_nodes[...] = value.astype(BF16)


def round_up(value, unit):
    return -(-value // unit) * unit


def per_device(
    nodes, edges, senders, receivers, counts, w_edge_in, w_edge_hid, w_edge_out, edge_bias,
    edge_gain, edge_shift, w_node_in, w_node_hid, w_node_out, node_bias, node_gain, node_shift,
):
    rows, cols, latent = nodes.shape
    bands, slots = edges.shape[2:4]
    band_rows = rows // bands
    num_rows, num_cols = lax.axis_size("row"), lax.axis_size("col")
    tile_edges = edges.reshape(bands, slots, latent)
    tile_send = senders.reshape(bands, slots)
    tile_recv = receivers.reshape(bands, slots)
    tile_counts = counts.reshape(bands)
    flat = nodes.reshape(rows * cols, latent)

    step = 2 if bands % 2 == 0 else 1
    stages = num_cols + num_rows - 2
    norm, halo_row, halo_col = pl.pallas_call(
        functools.partial(exchange_kernel, num_rows, num_cols, step),
        grid=(bands // step,),
        in_specs=[SMEM, pl.BlockSpec((step, slots, latent), lambda i: (i, 0, 0)), VMEM],
        out_specs=[VMEM] * 3,
        out_shape=[
            jax.ShapeDtypeStruct((8, latent), F32),
            jax.ShapeDtypeStruct((2, cols, latent), BF16),
            jax.ShapeDtypeStruct((2, rows + 2 * TAIL, latent), BF16),
        ],
        scratch_shapes=[
            pltpu.VMEM((2, cols, latent), BF16),
            pltpu.VMEM((2, rows + 2 * TAIL, latent), BF16),
            pltpu.VMEM((8, latent), F32),
            pltpu.VMEM((8, latent), F32),
            pltpu.VMEM((8, latent), F32),
            pltpu.VMEM((2, rows, latent), BF16),
            pltpu.VMEM((1, 3 * latent), F32),
            pltpu.VMEM((max(num_cols - 1, 1), 1, 3 * latent), F32),
            pltpu.VMEM((1, 3 * latent), F32),
            pltpu.VMEM((max(num_rows - 1, 1), 1, 3 * latent), F32),
            pltpu.SemaphoreType.DMA((8,)),
            pltpu.SemaphoreType.DMA((8,)),
            pltpu.SemaphoreType.DMA((stages,)),
            pltpu.SemaphoreType.DMA((stages,)),
        ],
        compiler_params=pltpu.CompilerParams(collective_id=0, has_side_effects=True),
        name="exchange",
    )(tile_counts, tile_edges, nodes)

    band_nodes = band_rows * cols
    table = round_up((band_rows + 2) * cols + 16, 128)
    out_edges, out_nodes = pl.pallas_call(
        functools.partial(main_kernel, band_rows, cols),
        grid=(bands,),
        in_specs=[SMEM, pl.BlockSpec((1, slots, latent), lambda i: (i, 0, 0))] + [VMEM] * 18,
        out_specs=[pl.BlockSpec((1, slots, latent), lambda i: (i, 0, 0)), VMEM],
        out_shape=[
            jax.ShapeDtypeStruct((bands, slots, latent), BF16),
            jax.ShapeDtypeStruct((rows * cols, latent), BF16),
        ],
        scratch_shapes=[
            pltpu.VMEM(((rows + 2) * cols, latent), BF16),
            pltpu.VMEM((rows + 2 * TAIL, latent), F32),
            pltpu.VMEM((rows + 2 * TAIL, latent), F32),
            pltpu.VMEM((rows * cols, latent), BF16),
            pltpu.VMEM((table + band_nodes + latent, latent), BF16),
            pltpu.VMEM((2 * latent, 2 * latent), BF16),
            pltpu.VMEM((2 * latent, 2 * latent), BF16),
            pltpu.VMEM((2 * latent, 2 * latent), BF16),
            pltpu.VMEM((rows * cols, latent), BF16),
        ],
        name="processor",
    )(
        tile_counts, tile_edges, tile_send, tile_recv, flat, halo_row, halo_col, norm,
        w_edge_in, w_edge_hid, w_edge_out, edge_bias, edge_gain.reshape(1, latent),
        edge_shift.reshape(1, latent), w_node_in, w_node_hid, w_node_out, node_bias,
        node_gain.reshape(1, latent), node_shift.reshape(1, latent),
    )
    return out_nodes.reshape(rows, cols, latent), out_edges.reshape(edges.shape)


def solution(mesh):
    tile = ("row", "col")
    in_specs = (
        P(*tile, None),
        P(*tile, None, None, None),
        P(*tile, None, None),
        P(*tile, None, None),
        P(*tile, None),
    ) + (P(),) * 12
    out_specs = (P(*tile, None), P(*tile, None, None, None))
    return jax.shard_map(
        per_device, mesh=mesh, in_specs=in_specs, out_specs=out_specs, check_vma=False
    )
```

```python
import functools

import jax
import jax.numpy as jnp
from jax import lax
from jax.experimental import pallas as pl
from jax.experimental.pallas import tpu as pltpu
from jax.sharding import PartitionSpec as P

MESH = pl.DeviceIdType.MESH
EPS = 1e-05
TAIL = 16
F32 = jnp.float32
BF16 = jnp.bfloat16
VMEM = pl.BlockSpec(memory_space=pltpu.VMEM)
SMEM = pl.BlockSpec(memory_space=pltpu.SMEM)


def dot(a, b):
    return jnp.dot(a, b, preferred_element_type=F32)


def combine(tiles, latent):
    parts = [[tile[:, k * latent : (k + 1) * latent] for k in range(3)] for tile in tiles]
    number = sum(n for _, _, n in parts)
    mean = sum(n * m for m, _, n in parts) / number
    power = sum(p + n * (m - mean) * (m - mean) for m, p, n in parts)
    return mean, power, number


def exchange_kernel(
    num_rows, num_cols, bands_step, counts, edges, nodes, norm, row_out, col_out,
    halo_row, halo_col, acc_sum, acc_sq, shift, col_edge, stats, first, middle, second,
    send_sem, recv_sem, stat_send, stat_recv,
):
    step, steps = pl.program_id(0), pl.num_programs(0)
    r, c = lax.axis_index("row"), lax.axis_index("col")
    slots, latent = edges.shape[1:]
    length, cols = nodes.shape[0:2]

    def at(dr, dc):
        return (lax.rem(r + dr + num_rows, num_rows), lax.rem(c + dc + num_cols, num_cols))

    near = [(0, k) for k in range(1, num_cols)] + [(k, 0) for k in range(1, num_rows)]
    peers = near + [(1, 1), (1, -1), (-1, 1), (-1, -1)]
    barrier = pltpu.get_barrier_semaphore()

    def copy_of(src, dst, ss, rs, dr, dc):
        return pltpu.make_async_remote_copy(
            src_ref=src, dst_ref=dst, send_sem=ss, recv_sem=rs,
            device_id=at(dr, dc), device_id_type=MESH,
        )

    top, low = pl.ds(0, TAIL), pl.ds(length - TAIL, TAIL)
    plan = [
        (col_edge.at[1], halo_col.at[0, pl.ds(TAIL, length)], 0, 1),
        (col_edge.at[0], halo_col.at[1, pl.ds(TAIL, length)], 0, -1),
        (nodes.at[length - 1], halo_row.at[0], 1, 0),
        (nodes.at[0], halo_row.at[1], -1, 0),
        (col_edge.at[1, low], halo_col.at[0, top], 1, 1),
        (col_edge.at[1, top], halo_col.at[0, pl.ds(TAIL + length, TAIL)], -1, 1),
        (col_edge.at[0, low], halo_col.at[1, top], 1, -1),
        (col_edge.at[0, top], halo_col.at[1, pl.ds(TAIL + length, TAIL)], -1, -1),
    ]

    def halo():
        return [
            copy_of(src, dst, send_sem.at[i], recv_sem.at[i], dr, dc)
            for i, (src, dst, dr, dc) in enumerate(plan)
        ]

    @pl.when(step == 0)
    def _():
        for dr, dc in peers:
            pl.semaphore_signal(barrier, inc=1, device_id=at(dr, dc), device_id_type=MESH)
        shift[...] = jnp.broadcast_to(edges[0, 0:TAIL, :].astype(F32)[0:1], shift.shape)
        acc_sum[...] = jnp.zeros_like(acc_sum)
        acc_sq[...] = jnp.zeros_like(acc_sq)
        flat = nodes[...].reshape(length * cols, latent)
        line = lax.broadcasted_iota(jnp.int32, (length, length * cols), 0) * cols
        place = lax.broadcasted_iota(jnp.int32, (length, length * cols), 1)
        for side, offset in enumerate((0, cols - 1)):
            pick = jnp.where(place == line + offset, 1.0, 0.0).astype(BF16)
            col_edge[side] = dot(pick, flat).astype(BF16)

    base = shift[0:1, :]
    total, square = acc_sum[...], acc_sq[...]
    group = 64
    for k in range(bands_step):
        count = counts[step * bands_step + k]
        for lo in range(0, slots, group):
            moved = edges[k, lo : lo + group, :].astype(F32) - base
            if lo + group > slots // 2:
                rows = lax.broadcasted_iota(jnp.int32, (group, latent), 0) + lo
                moved = jnp.where(rows < count, moved, 0.0)
            total += jnp.sum(moved.reshape(-1, 8, latent), axis=0)
            square += jnp.sum((moved * moved).reshape(-1, 8, latent), axis=0)
    acc_sum[...] = total
    acc_sq[...] = square

    @pl.when(step == steps - 1)
    def _():
        amount = counts[0]
        for k in range(1, counts.shape[0]):
            amount = amount + counts[k]
        amount = jnp.full((1, latent), amount.astype(F32))
        offset = jnp.sum(acc_sum[...], axis=0, keepdims=True) / amount
        spare = jnp.sum(acc_sq[...], axis=0, keepdims=True) - offset * offset * amount
        stats[...] = jnp.concatenate([base + offset, spare, amount], axis=1)
        stage = [
            copy_of(stats, first.at[k - 1], stat_send.at[k - 1], stat_recv.at[k - 1], 0, k)
            for k in range(1, num_cols)
        ]
        pl.semaphore_wait(barrier, len(peers))
        for copy in stage:
            copy.start()
        for copy in halo():
            copy.start()
        for copy in stage:
            copy.wait()
        merged = combine([stats[...]] + [first[k] for k in range(num_cols - 1)], latent)
        middle[...] = jnp.concatenate(merged, axis=1)
        past = num_cols - 1
        stage = [
            copy_of(
                middle, second.at[k - 1], stat_send.at[past + k - 1],
                stat_recv.at[past + k - 1], k, 0,
            )
            for k in range(1, num_rows)
        ]
        for copy in stage:
            copy.start()
        for copy in halo():
            copy.wait()
        row_out[...] = halo_row[...]
        col_out[...] = halo_col[...]
        for copy in stage:
            copy.wait()
        mean, power, number = combine(
            [middle[...]] + [second[k] for k in range(num_rows - 1)], latent
        )
        spread = lax.rsqrt(jnp.maximum(power / number, 0.0) + EPS)
        norm[...] = jnp.concatenate([mean, spread, jnp.zeros((6, latent), F32)], axis=0)


def twice(w):
    zero = jnp.zeros_like(w)
    return jnp.concatenate(
        [jnp.concatenate([w, zero], axis=1), jnp.concatenate([zero, w], axis=1)], axis=0
    )


def centred(w):
    wide = w.astype(F32)
    return wide - jnp.mean(wide, axis=-1, keepdims=True)


def main_kernel(
    band_rows, cols, chunks, even_last, counts, edges, send_all, recv_all, nodes, halo_row, halo_col, norm,
    w_in, w_hid, w_out, bias, gain, shift, v_in, v_hid, v_out, n_bias, n_gain, n_shift,
    new_edges, new_nodes,
    proj_send, proj_left, proj_right, proj_recv, mixed, two_hid, two_out, two_mean, gathered,
    one_even, norm_even, one_odd, norm_odd,
):
    step, bands = pl.program_id(0), pl.num_programs(0) - 1
    slots, latent = edges.shape[1:]
    band_nodes = band_rows * cols
    window_rows = band_rows + 2
    main = window_rows * cols
    table = mixed.shape[0] - band_nodes - latent
    half = slots // 2
    length = half // chunks
    even, odd = (one_even, norm_even), (one_odd, norm_odd)

    def spread_rows(index, lo):
        return jnp.broadcast_to(index[:, lo : lo + 128], (128, 128)).T

    def pick(values, width, offset=0):
        lanes = lax.broadcasted_iota(jnp.int32, (values.shape[0], width), 1) + offset
        return jnp.where(values == lanes, 1.0, 0.0).astype(BF16)

    def head(store):
        one, normed = store
        band = step
        start = pl.multiple_of(band * band_nodes, band_nodes)
        side = TAIL - 1 + band * band_rows
        mixed[0:main, :] = proj_send[pl.ds(start, main), :]
        mixed[main : main + 16, :] = jnp.concatenate(
            [proj_left[pl.ds(side, 8), :], proj_right[pl.ds(side, 8), :]], axis=0
        ).astype(BF16)
        mixed[table : table + band_nodes, :] = proj_recv[pl.ds(start, band_nodes), :]
        weights = mixed[...]
        send = send_all[pl.ds(band, 1), :]
        recv = recv_all[pl.ds(band, 1), :]
        row = sum((send >= (cols + 2) * k).astype(jnp.int32) for k in range(1, window_rows))
        col = send - (cols + 2) * row
        place = jnp.where(
            col == 0, main + row, jnp.where(col == cols + 1, main + 8 + row, row * cols + col - 1)
        )
        mean, spread = norm[0:1, :], norm[1:2, :]

        def run(chunk):
            pieces = []
            for part in range(2):
                first = part * half + chunk * length
                for lo in range(first, first + length, 128):
                    s, q = spread_rows(place, lo), spread_rows(recv, lo)
                    hot = [pick(s, 128, off) for off in range(0, table, 128)]
                    hot += [pick(q, 128, off) for off in range(0, band_nodes, 128)]
                    block = edges[0, lo : lo + 128, :].astype(F32)
                    value = ((block - mean) * spread).astype(BF16)
                    normed[lo : lo + 128, :] = value
                    pieces.append(jnp.concatenate(hot + [value], axis=1))
            result = dot(jnp.concatenate(pieces, axis=0), weights)
            result = jnp.maximum(result, 0.0).astype(BF16)
            lines = slice(chunk * length, (chunk + 1) * length)
            one[lines, :] = jnp.concatenate([result[:length], result[length:]], axis=1)

        return run

    def tail(store):
        one, normed = store
        band = step - 1
        start = pl.multiple_of(band * band_nodes, band_nodes)
        recv = recv_all[pl.ds(band, 1), :]
        count = counts[band]
        bias_hid = jnp.concatenate([bias[1:2, :]] * 2, axis=1)
        bias_msg = bias[2:3, :] - jnp.mean(bias[2:3, :], axis=-1, keepdims=True)
        bias_out = jnp.concatenate([bias_msg] * 2, axis=1)
        sums = []

        def run(chunk):
            lines = slice(chunk * length, (chunk + 1) * length)
            two = jnp.maximum(dot(one[lines, :], two_hid[...]) + bias_hid, 0.0).astype(BF16)
            message = dot(two, two_out[...]) + bias_out
            power = dot((message * message).astype(BF16), two_mean[...])
            unit = message * lax.rsqrt(power + EPS)
            fresh, picks = [], []
            for part in range(2):
                lo = part * half + chunk * length
                value = normed[lo : lo + length, :].astype(F32) + shift[...]
                value = value + unit[:, part * latent : (part + 1) * latent] * gain[...]
                if lo + length > slots // 2:
                    rows = lax.broadcasted_iota(jnp.int32, (length, latent), 0) + lo
                    value = jnp.where(rows < count, value, 0.0)
                value = value.astype(BF16)
                new_edges[0, lo : lo + length, :] = value
                fresh.append(value)
                places = lax.broadcasted_iota(jnp.int32, (band_nodes, length), 0)
                hit = places == recv[:, lo : lo + length]
                picks.append(jnp.where(hit, 1.0, 0.0).astype(BF16))
            fresh, picks = jnp.concatenate(fresh, axis=0), jnp.concatenate(picks, axis=1)
            sums.append(dot(picks, fresh))
            if chunk == chunks - 1:
                gathered[pl.ds(start, band_nodes), :] = sum(sums).astype(BF16)

        return run

    def work(before, after):
        runs = [tail(before)] if before else []
        runs += [head(after)] if after else []
        for chunk in range(chunks):
            for run in runs:
                run(chunk)

    @pl.when(step == 0)
    def _():
        w_send = w_in[latent : 2 * latent, :]
        w_recv = w_in[2 * latent :, :]
        total = nodes.shape[0]
        proj_send[0:cols, :] = dot(halo_row[0], w_send).astype(BF16)
        proj_send[cols : cols + total, :] = dot(nodes[...], w_send).astype(BF16)
        proj_send[cols + total :, :] = dot(halo_row[1], w_send).astype(BF16)
        proj_left[...] = dot(halo_col[0], w_send)
        proj_right[...] = dot(halo_col[1], w_send)
        proj_recv[...] = (dot(nodes[...], w_recv) + bias[0:1, :]).astype(BF16)
        mixed[...] = jnp.zeros_like(mixed)
        mixed[table + band_nodes :, :] = w_in[0:latent, :]
        two_hid[...] = twice(w_hid[...])
        two_out[...] = twice(centred(w_out[...]).astype(BF16))
        two_mean[...] = twice(jnp.full((latent, latent), 1.0 / latent, BF16))
        work(None, even)

    inside = (step > 0) & (step < bands)

    @pl.when(inside & (step % 2 == 1))
    def _():
        work(even, odd)

    @pl.when(inside & (step % 2 == 0))
    def _():
        work(odd, even)

    @pl.when(step == bands)
    def _():
        work(even if even_last else odd, None)
        own = nodes[...]
        middle = own.shape[0] // 2

        def pair(value):
            return jnp.concatenate([value[:middle], value[middle:]], axis=1)

        def wide(row):
            return jnp.concatenate([row, row], axis=1)

        joined = jnp.concatenate([own, gathered[...]], axis=1)
        node_one = jnp.maximum(dot(joined, v_in[...]) + n_bias[0:1, :], 0.0).astype(BF16)
        node_two = dot(pair(node_one), twice(v_hid[...])) + wide(n_bias[1:2, :])
        node_two = jnp.maximum(node_two, 0.0).astype(BF16)
        out_bias = n_bias[2:3, :] - jnp.mean(n_bias[2:3, :], axis=-1, keepdims=True)
        note = dot(node_two, twice(centred(v_out[...]).astype(BF16))) + wide(out_bias)
        level = dot((note * note).astype(BF16), two_mean[...])
        unit = note * lax.rsqrt(level + EPS)
        for part in range(2):
            rows = slice(part * middle, (part + 1) * middle)
            value = own[rows].astype(F32) + n_shift[...]
            value = value + unit[:, part * latent : (part + 1) * latent] * n_gain[...]
            new_nodes[rows, :] = value.astype(BF16)


def round_up(value, unit):
    return -(-value // unit) * unit


def per_device(
    nodes, edges, senders, receivers, counts, w_edge_in, w_edge_hid, w_edge_out, edge_bias,
    edge_gain, edge_shift, w_node_in, w_node_hid, w_node_out, node_bias, node_gain, node_shift,
):
    rows, cols, latent = nodes.shape
    bands, slots = edges.shape[2:4]
    band_rows = rows // bands
    num_rows, num_cols = lax.axis_size("row"), lax.axis_size("col")
    tile_edges = edges.reshape(bands, slots, latent)
    tile_send = senders.reshape(bands, slots)
    tile_recv = receivers.reshape(bands, slots)
    tile_counts = counts.reshape(bands)
    flat = nodes.reshape(rows * cols, latent)

    step = 2 if bands % 2 == 0 else 1
    stages = num_cols + num_rows - 2
    norm, halo_row, halo_col = pl.pallas_call(
        functools.partial(exchange_kernel, num_rows, num_cols, step),
        grid=(bands // step,),
        in_specs=[SMEM, pl.BlockSpec((step, slots, latent), lambda i: (i, 0, 0)), VMEM],
        out_specs=[VMEM] * 3,
        out_shape=[
            jax.ShapeDtypeStruct((8, latent), F32),
            jax.ShapeDtypeStruct((2, cols, latent), BF16),
            jax.ShapeDtypeStruct((2, rows + 2 * TAIL, latent), BF16),
        ],
        scratch_shapes=[
            pltpu.VMEM((2, cols, latent), BF16),
            pltpu.VMEM((2, rows + 2 * TAIL, latent), BF16),
            pltpu.VMEM((8, latent), F32),
            pltpu.VMEM((8, latent), F32),
            pltpu.VMEM((8, latent), F32),
            pltpu.VMEM((2, rows, latent), BF16),
            pltpu.VMEM((1, 3 * latent), F32),
            pltpu.VMEM((max(num_cols - 1, 1), 1, 3 * latent), F32),
            pltpu.VMEM((1, 3 * latent), F32),
            pltpu.VMEM((max(num_rows - 1, 1), 1, 3 * latent), F32),
            pltpu.SemaphoreType.DMA((8,)),
            pltpu.SemaphoreType.DMA((8,)),
            pltpu.SemaphoreType.DMA((stages,)),
            pltpu.SemaphoreType.DMA((stages,)),
        ],
        compiler_params=pltpu.CompilerParams(collective_id=0, has_side_effects=True),
        name="exchange",
    )(tile_counts, tile_edges, nodes)

    band_nodes = band_rows * cols
    table = round_up((band_rows + 2) * cols + 16, 128)
    out_edges, out_nodes = pl.pallas_call(
        functools.partial(main_kernel, band_rows, cols, 1, bands % 2 == 1),
        grid=(bands + 1,),
        in_specs=[
            SMEM,
            pl.BlockSpec((1, slots, latent), lambda i: (jnp.minimum(i, bands - 1), 0, 0)),
        ] + [VMEM] * 18,
        out_specs=[
            pl.BlockSpec((1, slots, latent), lambda i: (jnp.maximum(i - 1, 0), 0, 0)), VMEM,
        ],
        out_shape=[
            jax.ShapeDtypeStruct((bands, slots, latent), BF16),
            jax.ShapeDtypeStruct((rows * cols, latent), BF16),
        ],
        scratch_shapes=[
            pltpu.VMEM(((rows + 2) * cols, latent), BF16),
            pltpu.VMEM((rows + 2 * TAIL, latent), F32),
            pltpu.VMEM((rows + 2 * TAIL, latent), F32),
            pltpu.VMEM((rows * cols, latent), BF16),
            pltpu.VMEM((table + band_nodes + latent, latent), BF16),
            pltpu.VMEM((2 * latent, 2 * latent), BF16),
            pltpu.VMEM((2 * latent, 2 * latent), BF16),
            pltpu.VMEM((2 * latent, 2 * latent), BF16),
            pltpu.VMEM((rows * cols, latent), BF16),
        ] + [
            pltpu.VMEM((slots // 2, 2 * latent), BF16),
            pltpu.VMEM((slots, latent), BF16),
        ] * 2,
        name="processor",
    )(
        tile_counts, tile_edges, tile_send, tile_recv, flat, halo_row, halo_col, norm,
        w_edge_in, w_edge_hid, w_edge_out, edge_bias, edge_gain.reshape(1, latent),
        edge_shift.reshape(1, latent), w_node_in, w_node_hid, w_node_out, node_bias,
        node_gain.reshape(1, latent), node_shift.reshape(1, latent),
    )
    return out_nodes.reshape(rows, cols, latent), out_edges.reshape(edges.shape)


def solution(mesh):
    tile = ("row", "col")
    in_specs = (
        P(*tile, None),
        P(*tile, None, None, None),
        P(*tile, None, None),
        P(*tile, None, None),
        P(*tile, None),
    ) + (P(),) * 12
    out_specs = (P(*tile, None), P(*tile, None, None, None))
    return jax.shard_map(
        per_device, mesh=mesh, in_specs=in_specs, out_specs=out_specs, check_vma=False
    )
```
